64 devices in a mesh: data: 4 (over x, y), model: 16 (over z, core).
Axes of the slice: x: 2, y: 2, z: 8, core: 2. Of those that a mesh axis runs over, the one named last changes fastest.
The devices are a block of a 4x4x8 slice.
Arguments:
- hidden_in: bfloat16 [4, 4096, 1536], P('data', 'model'), parts along dimension 0
- seg_ids: int32 [4, 4096], P('data'), parts along dimension 0
- gain_attn: bfloat16 [1536], replicated
- w_qkv: bfloat16 [1536, 16, 3, 96], P(None, 'model')
- w_out: bfloat16 [16, 96, 1536], P('model')
- gain_mlp: bfloat16 [1536], replicated
- w_up: bfloat16 [1536, 6144], P(None, 'model')
- w_down: bfloat16 [6144, 1536], P('model')
- grad_out: bfloat16 [4, 4096, 1536], P('data', 'model'), parts along dimension 0
Outputs:
- output 1: bfloat16 [4, 4096, 1536], P('data', 'model'), parts along dimension 0
- output 2: bfloat16 [4, 4096, 1536], P('data', 'model'), parts along dimension 0
- output 3: bfloat16 [6144, 16, 3, 96], P('data', 'model'), parts along dimension 0
- output 4: bfloat16 [64, 96, 1536], P(('data', 'model')), parts along dimension 0
- output 5: bfloat16 [6144, 6144], P('data', 'model'), parts along dimension 0
- output 6: bfloat16 [24576, 1536], P(('data', 'model')), parts along dimension 0
- output 7: bfloat16 [6144], P('data'), parts along dimension 0
- output 8: bfloat16 [6144], P('data'), parts along dimension 0
There are 4 independent parts. The reference program is written for one: setup_inputs(seed, part) draws one part's arguments, and reference() takes and returns one part's arrays. A program takes and returns all parts, laid end to end along the dimension named above; an argument that names none is the same for every part.
All inputs are finite; a program needn't handle non-finite values.
Results may differ from the reference program's by a relative error of at most 0.02.
Values are sent between devices in bfloat16 or wider.
A program may use at most 768 MiB of HBM per device.

```python
import jax
import jax.numpy as jnp
from jax import lax

BATCH = 1
SEQ_LEN = 4096
HIDDEN = 1536
HEADS = 16
HEAD_DIM = 96
FFN_DIM = 6144

LN_EPS = 1e-5
TOKENS = BATCH * SEQ_LEN
QKV_WIDTH = 3 * HEADS * HEAD_DIM
ATTN_WIDTH = HEADS * HEAD_DIM


def draw_segments(seg_key):
    cut_points = jax.random.randint(seg_key, (BATCH, 3), 1, SEQ_LEN)
    positions = jnp.arange(SEQ_LEN)
    return jnp.sum(positions[None, :, None] >= cut_points[:, None, :], axis=-1).astype(jnp.int32)


def normal_array(rand_key, shape, scale):
    return (scale * jax.random.normal(rand_key, shape, jnp.float32)).astype(jnp.bfloat16)


def setup_inputs(seed: int = 0, part: int = 0) -> dict:
    root_key = jax.random.key(seed)
    shared = jax.random.split(root_key, 6)
    part_keys = jax.random.split(jax.random.fold_in(root_key, part), 3)
    return {
        'hidden_in': normal_array(part_keys[0], (BATCH, SEQ_LEN, HIDDEN), 1.0),
        'seg_ids': draw_segments(part_keys[2]),
        'gain_attn': (1.0 + 0.3 * jax.random.normal(shared[0], (HIDDEN,), jnp.float32)).astype(jnp.bfloat16),
        'w_qkv': normal_array(shared[2], (HIDDEN, HEADS, 3, HEAD_DIM), 1.5 * HIDDEN ** -0.5),
        'w_out': normal_array(shared[3], (HEADS, HEAD_DIM, HIDDEN), 1.5 * ATTN_WIDTH ** -0.5),
        'gain_mlp': (1.0 + 0.3 * jax.random.normal(shared[1], (HIDDEN,), jnp.float32)).astype(jnp.bfloat16),
        'w_up': normal_array(shared[4], (HIDDEN, FFN_DIM), HIDDEN ** -0.5),
        'w_down': normal_array(shared[5], (FFN_DIM, HIDDEN), FFN_DIM ** -0.5),
        'grad_out': normal_array(part_keys[1], (BATCH, SEQ_LEN, HIDDEN), 1.0),
    }


def layer_norm(x_f32, gain_f32):
    mean_val = jnp.mean(x_f32, axis=-1, keepdims=True)
    centered = x_f32 - mean_val
    variance = jnp.mean(centered * centered, axis=-1, keepdims=True)
    return centered * lax.rsqrt(variance + LN_EPS) * gain_f32


def gelu_tanh(pre_act):
    return jax.nn.gelu(pre_act, approximate=True)


def head_probs(q_head, k_head, attn_mask):
    scores = jnp.einsum('bqd,bkd->bqk', q_head.astype(jnp.float32), k_head.astype(jnp.float32)) * HEAD_DIM ** -0.5
    return jax.nn.softmax(jnp.where(attn_mask, scores, -1e30), axis=-1)


def head_forward(head_qkv, attn_mask):
    attn_prob = head_probs(head_qkv[0], head_qkv[1], attn_mask)
    prob_lo = attn_prob.astype(jnp.bfloat16).astype(jnp.float32)
    return jnp.einsum('bqk,bkd->bqd', prob_lo, head_qkv[2].astype(jnp.float32)).astype(jnp.bfloat16)


def head_backward(head_qkv, head_out, d_head, attn_mask):
    q_head = head_qkv[0].astype(jnp.float32)
    k_head = head_qkv[1].astype(jnp.float32)
    v_head = head_qkv[2].astype(jnp.float32)
    attn_prob = head_probs(head_qkv[0], head_qkv[1], attn_mask)
    d_out = d_head.astype(jnp.float32)
    d_prob = jnp.einsum('bqd,bkd->bqk', d_out, v_head)
    row_delta = jnp.sum(d_out * head_out.astype(jnp.float32), axis=-1, keepdims=True)
    d_scores = (attn_prob * (d_prob - row_delta) * HEAD_DIM ** -0.5).astype(jnp.bfloat16).astype(jnp.float32)
    d_q = jnp.einsum('bqk,bkd->bqd', d_scores, k_head).astype(jnp.bfloat16)
    d_k = jnp.einsum('bqk,bqd->bkd', d_scores, q_head).astype(jnp.bfloat16)
    prob_lo = attn_prob.astype(jnp.bfloat16).astype(jnp.float32)
    d_v = jnp.einsum('bqk,bqd->bkd', prob_lo, d_out).astype(jnp.bfloat16)
    return jnp.stack([d_q, d_k, d_v])


def reference(hidden_in, seg_ids, gain_attn, w_qkv, w_out, gain_mlp, w_up, w_down, grad_out):
    x_rows = hidden_in.reshape(TOKENS, HIDDEN).astype(jnp.float32)
    ln1_out, ln1_vjp = jax.vjp(layer_norm, x_rows, gain_attn.astype(jnp.float32))
    attn_in = ln1_out.astype(jnp.bfloat16)
    w_qkv_flat = w_qkv.reshape(HIDDEN, QKV_WIDTH)
    qkv_flat = jnp.dot(attn_in, w_qkv_flat, preferred_element_type=jnp.float32).astype(jnp.bfloat16)
    qkv_heads = jnp.transpose(qkv_flat.reshape(BATCH, SEQ_LEN, HEADS, 3, HEAD_DIM), (2, 3, 0, 1, 4))
    positions = jnp.arange(SEQ_LEN)
    attn_mask = (positions[None, :, None] >= positions[None, None, :]) & (seg_ids[:, :, None] == seg_ids[:, None, :])
    attn_heads = lax.map(lambda head_qkv: head_forward(head_qkv, attn_mask), qkv_heads)
    attn_cat = jnp.transpose(attn_heads, (1, 2, 0, 3)).reshape(TOKENS, ATTN_WIDTH)
    w_out_flat = w_out.reshape(ATTN_WIDTH, HIDDEN)
    attn_sum = jnp.dot(attn_cat, w_out_flat, preferred_element_type=jnp.float32).astype(jnp.bfloat16)
    mid_rows = (x_rows + attn_sum.astype(jnp.float32)).astype(jnp.bfloat16)
    ln2_out, ln2_vjp = jax.vjp(layer_norm, mid_rows.astype(jnp.float32), gain_mlp.astype(jnp.float32))
    mlp_in = ln2_out.astype(jnp.bfloat16)
    pre_act = jnp.dot(mlp_in, w_up, preferred_element_type=jnp.float32)
    act_f32, gelu_vjp = jax.vjp(gelu_tanh, pre_act)
    act_lo = act_f32.astype(jnp.bfloat16)
    mlp_sum = jnp.dot(act_lo, w_down, preferred_element_type=jnp.float32).astype(jnp.bfloat16)
    out_rows = (mid_rows.astype(jnp.float32) + mlp_sum.astype(jnp.float32)).astype(jnp.bfloat16)
    dy_rows = grad_out.reshape(TOKENS, HIDDEN)
    d_act = jnp.dot(dy_rows, w_down.T, preferred_element_type=jnp.float32)
    d_pre = gelu_vjp(d_act)[0].astype(jnp.bfloat16)
    g_down = jnp.dot(act_lo.T, dy_rows, preferred_element_type=jnp.float32).astype(jnp.bfloat16)
    d_mlp_in = jnp.dot(d_pre, w_up.T, preferred_element_type=jnp.float32).astype(jnp.bfloat16)
    g_up = jnp.dot(mlp_in.T, d_pre, preferred_element_type=jnp.float32).astype(jnp.bfloat16)
    d_mid_ln, d_gain_mlp = ln2_vjp(d_mlp_in.astype(jnp.float32))
    d_mid = (dy_rows.astype(jnp.float32) + d_mid_ln).astype(jnp.bfloat16)
    d_attn_cat = jnp.dot(d_mid, w_out_flat.T, preferred_element_type=jnp.float32).astype(jnp.bfloat16)
    g_out = jnp.dot(attn_cat.T, d_mid, preferred_element_type=jnp.float32).astype(jnp.bfloat16)
    d_heads = jnp.transpose(d_attn_cat.reshape(BATCH, SEQ_LEN, HEADS, HEAD_DIM), (2, 0, 1, 3))
    d_qkv_heads = lax.map(lambda head_args: head_backward(head_args[0], head_args[1], head_args[2], attn_mask), (qkv_heads, attn_heads, d_heads))
    d_qkv = jnp.transpose(d_qkv_heads, (2, 3, 0, 1, 4)).reshape(TOKENS, QKV_WIDTH)
    d_attn_in = jnp.dot(d_qkv, w_qkv_flat.T, preferred_element_type=jnp.float32).astype(jnp.bfloat16)
    g_qkv = jnp.dot(attn_in.T, d_qkv, preferred_element_type=jnp.float32).astype(jnp.bfloat16)
    d_x_ln, d_gain_attn = ln1_vjp(d_attn_in.astype(jnp.float32))
    grad_in = (d_mid.astype(jnp.float32) + d_x_ln).astype(jnp.bfloat16)
    return (out_rows.reshape(BATCH, SEQ_LEN, HIDDEN), grad_in.reshape(BATCH, SEQ_LEN, HIDDEN), g_qkv.reshape(HIDDEN, HEADS, 3, HEAD_DIM), g_out.reshape(HEADS, HEAD_DIM, HIDDEN), g_up, g_down, d_gain_attn.astype(jnp.bfloat16), d_gain_mlp.astype(jnp.bfloat16))
```

```python
import functools

import jax
import jax.numpy as jnp
from jax import lax
from jax.experimental import pallas as pl
from jax.experimental.pallas import tpu as pltpu
from jax.sharding import PartitionSpec as P

LN_EPS = 1e-5


NEG = -1e30
LOG2E = 1.4426950408889634


def visible_from(pos, cuts):
    first = jnp.zeros_like(pos)
    for n in range(3):
        first = jnp.where(pos >= cuts[n], jnp.maximum(first, cuts[n]), first)
    return first


def attn_fwd_body(dim, blk, cuts_ref, qkv_ref, out_ref, lse_ref, k_nat, m_ref, l_ref, acc):
    seq_len = qkv_ref.shape[1]
    mul = dim ** -0.5 * LOG2E
    cuts = [cuts_ref[n] for n in range(3)]

    def span(n):
        return pl.ds(pl.multiple_of(n * blk, blk), blk)

    @pl.loop(0, seq_len // blk)
    def _(n):
        k_nat[span(n), :] = qkv_ref[dim:2 * dim, span(n)].T

    @pl.loop(0, seq_len // blk)
    def _(i):
        q_t = qkv_ref[0:dim, span(i)]
        q_pos = i * blk + lax.broadcasted_iota(jnp.int32, (1, blk), 1)
        q_first = visible_from(q_pos, cuts)

        def block(j, kind):
            scores = jnp.dot(k_nat[span(j), :], q_t, preferred_element_type=jnp.float32) * mul
            if kind:
                k_pos = j * blk + lax.broadcasted_iota(jnp.int32, (blk, blk), 0)
                seen = k_pos >= q_first
                if kind == 2:
                    seen = seen & (k_pos <= q_pos)
                scores = jnp.where(seen, scores, NEG)
            top = jnp.max(scores, axis=0, keepdims=True)
            v_t = qkv_ref[2 * dim:3 * dim, span(j)]
            if kind == 2:
                prob = jnp.exp2(scores - top)
                m_ref[...] = top
                l_ref[...] = jnp.sum(prob, axis=0, keepdims=True)
                acc[...] = jnp.dot(v_t, prob.astype(jnp.bfloat16), preferred_element_type=jnp.float32)
            else:
                old = m_ref[...]
                top = jnp.maximum(old, top)
                prob = jnp.exp2(scores - top)
                fade = jnp.exp2(old - top)
                m_ref[...] = top
                l_ref[...] = l_ref[...] * fade + jnp.sum(prob, axis=0, keepdims=True)
                acc[...] = acc[...] * fade + jnp.dot(v_t, prob.astype(jnp.bfloat16), preferred_element_type=jnp.float32)

        block(i, 2)
        low = visible_from(i * blk, cuts) // blk
        whole = visible_from(i * blk + blk - 1, cuts)

        @pl.loop(low, i)
        def _(j):
            @pl.when(whole <= j * blk)
            def _():
                block(j, 0)

            @pl.when(whole > j * blk)
            def _():
                block(j, 1)

        total = l_ref[...]
        out_ref[:, span(i)] = (acc[...] / total).astype(jnp.bfloat16)
        lse_ref[:, span(i)] = m_ref[...] + jnp.log2(total)


def attn_fwd(qkv_t, cuts, dim, blk=512):
    seq_len = qkv_t.shape[1]
    return pl.pallas_call(
        functools.partial(attn_fwd_body, dim, blk),
        name="attn_fwd",
        out_shape=(jax.ShapeDtypeStruct((dim, seq_len), jnp.bfloat16), jax.ShapeDtypeStruct((1, seq_len), jnp.float32)),
        in_specs=[pl.BlockSpec(memory_space=pltpu.SMEM), pl.BlockSpec(memory_space=pltpu.VMEM)],
        out_specs=(pl.BlockSpec(memory_space=pltpu.VMEM),) * 2,
        scratch_shapes=[
            pltpu.VMEM((seq_len, dim), jnp.bfloat16),
            pltpu.VMEM((1, blk), jnp.float32),
            pltpu.VMEM((1, blk), jnp.float32),
            pltpu.VMEM((dim, blk), jnp.float32),
        ],
        cost_estimate=pl.CostEstimate(flops=2 * 2 * seq_len * seq_len * dim // 2, bytes_accessed=8 * dim * seq_len, transcendentals=seq_len * seq_len // 2),
        compiler_params=pltpu.CompilerParams(vmem_limit_bytes=40 << 20),
    )(cuts, qkv_t)


def attn_bwd_body(dim, blk, cuts_ref, qkv_ref, o_ref, do_ref, lse_ref, d_ref, k_nat, v_nat, delta, dq_acc, dk_acc, dv_acc):
    seq_len = qkv_ref.shape[1]
    scale = dim ** -0.5
    mul = scale * LOG2E
    count = seq_len // blk
    cuts = [cuts_ref[n] for n in range(3)]
    last_dims = (((1,), (1,)), ((), ()))

    def span(n):
        return pl.ds(pl.multiple_of(n * blk, blk), blk)

    @pl.loop(0, count)
    def _(n):
        k_nat[span(n), :] = qkv_ref[dim:2 * dim, span(n)].T
        v_nat[span(n), :] = qkv_ref[2 * dim:3 * dim, span(n)].T
        delta[:, span(n)] = jnp.sum(do_ref[:, span(n)].astype(jnp.float32) * o_ref[:, span(n)].astype(jnp.float32), axis=0, keepdims=True)
        dq_acc[:, span(n)] = jnp.zeros((dim, blk), jnp.float32)

    @pl.loop(0, count)
    def _(j):
        k_t = qkv_ref[dim:2 * dim, span(j)]

        def block(i, kind):
            q_t = qkv_ref[0:dim, span(i)]
            do_t = do_ref[:, span(i)]
            scores = jnp.dot(k_nat[span(j), :], q_t, preferred_element_type=jnp.float32) * mul
            prob = jnp.exp2(scores - lse_ref[:, span(i)])
            if kind:
                q_pos = i * blk + lax.broadcasted_iota(jnp.int32, (1, blk), 1)
                k_pos = j * blk + lax.broadcasted_iota(jnp.int32, (blk, blk), 0)
                seen = k_pos >= visible_from(q_pos, cuts)
                if kind == 2:
                    seen = seen & (k_pos <= q_pos)
                prob = jnp.where(seen, prob, 0.0)
            d_prob = jnp.dot(v_nat[span(j), :], do_t, preferred_element_type=jnp.float32)
            d_scores = (prob * (d_prob - delta[:, span(i)]) * scale).astype(jnp.bfloat16)
            d_v = lax.dot_general(prob.astype(jnp.bfloat16), do_t, last_dims, preferred_element_type=jnp.float32)
            d_k = lax.dot_general(d_scores, q_t, last_dims, preferred_element_type=jnp.float32)
            if kind == 2:
                dv_acc[...] = d_v
                dk_acc[...] = d_k
            else:
                dv_acc[...] += d_v
                dk_acc[...] += d_k
            dq_acc[:, span(i)] += jnp.dot(k_t, d_scores, preferred_element_type=jnp.float32)

        block(j, 2)

        @pl.loop(j + 1, count)
        def _(i):
            near = visible_from(i * blk, cuts)
            far = visible_from(i * blk + blk - 1, cuts)

            @pl.when(far <= j * blk)
            def _():
                block(i, 0)

            @pl.when((far > j * blk) & (near < (j + 1) * blk))
            def _():
                block(i, 1)

        d_ref[dim:2 * dim, span(j)] = dk_acc[...].T.astype(jnp.bfloat16)
        d_ref[2 * dim:3 * dim, span(j)] = dv_acc[...].T.astype(jnp.bfloat16)

    @pl.loop(0, count)
    def _(n):
        d_ref[0:dim, span(n)] = dq_acc[:, span(n)].astype(jnp.bfloat16)


def attn_bwd(qkv_t, o_t, do_t, lse, cuts, dim, blk=512):
    seq_len = qkv_t.shape[1]
    return pl.pallas_call(
        functools.partial(attn_bwd_body, dim, blk),
        name="attn_bwd",
        out_shape=jax.ShapeDtypeStruct((3 * dim, seq_len), jnp.bfloat16),
        in_specs=[pl.BlockSpec(memory_space=pltpu.SMEM)] + [pl.BlockSpec(memory_space=pltpu.VMEM)] * 4,
        out_specs=pl.BlockSpec(memory_space=pltpu.VMEM),
        scratch_shapes=[
            pltpu.VMEM((seq_len, dim), jnp.bfloat16),
            pltpu.VMEM((seq_len, dim), jnp.bfloat16),
            pltpu.VMEM((1, seq_len), jnp.float32),
            pltpu.VMEM((dim, seq_len), jnp.float32),
            pltpu.VMEM((blk, dim), jnp.float32),
            pltpu.VMEM((blk, dim), jnp.float32),
        ],
        cost_estimate=pl.CostEstimate(flops=2 * 5 * seq_len * seq_len * dim // 2, bytes_accessed=16 * dim * seq_len, transcendentals=seq_len * seq_len // 2),
        compiler_params=pltpu.CompilerParams(vmem_limit_bytes=40 << 20),
    )(cuts, qkv_t, o_t, do_t, lse)


def layer_norm(x_f32, gain_f32):
    mean_val = jnp.mean(x_f32, axis=-1, keepdims=True)
    centered = x_f32 - mean_val
    variance = jnp.mean(centered * centered, axis=-1, keepdims=True)
    return centered * lax.rsqrt(variance + LN_EPS) * gain_f32


def gelu_tanh(pre_act):
    return jax.nn.gelu(pre_act, approximate=True)


def dot(a, b, dims):
    return lax.dot_general(a, b, ((dims[0:1], dims[1:2]), ((), ())), preferred_element_type=jnp.float32)


def local_layer(hidden_in, seg_ids, gain_attn, w_qkv, w_out, gain_mlp, w_up, w_down, grad_out):
    dim = w_out.shape[1]
    hidden = w_out.shape[2]
    x = hidden_in[0]
    dy = grad_out[0]
    cuts = jnp.sum(seg_ids[0][None, :] < jnp.arange(1, 4, dtype=jnp.int32)[:, None], axis=1, dtype=jnp.int32)
    w_qkv_t = jnp.transpose(w_qkv, (1, 2, 3, 0)).reshape(3 * dim, hidden)
    w_o = w_out[0]
    x_f32 = x.astype(jnp.float32)
    ln1_out, ln1_vjp = jax.vjp(layer_norm, x_f32, gain_attn.astype(jnp.float32))
    attn_in = lax.all_gather(ln1_out.astype(jnp.bfloat16), 'model', axis=0, tiled=True)
    qkv_t = dot(w_qkv_t, attn_in, (1, 1)).astype(jnp.bfloat16)
    o_t, lse = attn_fwd(qkv_t, cuts, dim)
    attn_part = dot(o_t, w_o, (0, 0)).astype(jnp.bfloat16)
    attn_sum = lax.psum_scatter(attn_part, 'model', scatter_dimension=0, tiled=True)
    mid_loc = (x_f32 + attn_sum.astype(jnp.float32)).astype(jnp.bfloat16)
    ln2_out, ln2_vjp = jax.vjp(layer_norm, mid_loc.astype(jnp.float32), gain_mlp.astype(jnp.float32))
    mlp_in = lax.all_gather(ln2_out.astype(jnp.bfloat16), 'model', axis=0, tiled=True)
    pre_act = dot(mlp_in, w_up, (1, 0))
    act_f32, gelu_vjp = jax.vjp(gelu_tanh, pre_act)
    act_lo = act_f32.astype(jnp.bfloat16)
    mlp_part = dot(act_lo, w_down, (1, 0)).astype(jnp.bfloat16)
    mlp_sum = lax.psum_scatter(mlp_part, 'model', scatter_dimension=0, tiled=True)
    hidden_out = (mid_loc.astype(jnp.float32) + mlp_sum.astype(jnp.float32)).astype(jnp.bfloat16)
    grad_full = lax.all_gather(dy, 'model', axis=0, tiled=True)
    d_act = dot(grad_full, w_down, (1, 1))
    d_pre = gelu_vjp(d_act)[0].astype(jnp.bfloat16)
    g_down = dot(act_lo, grad_full, (0, 0)).astype(jnp.bfloat16)
    d_mlp_part = dot(d_pre, w_up, (1, 1)).astype(jnp.bfloat16)
    g_up = dot(mlp_in, d_pre, (0, 0)).astype(jnp.bfloat16)
    d_mlp_in = lax.psum_scatter(d_mlp_part, 'model', scatter_dimension=0, tiled=True)
    d_mid_ln, d_gain_mlp = ln2_vjp(d_mlp_in.astype(jnp.float32))
    d_mid = (dy.astype(jnp.float32) + d_mid_ln).astype(jnp.bfloat16)
    d_mid_full = lax.all_gather(d_mid, 'model', axis=0, tiled=True)
    do_t = dot(w_o, d_mid_full, (1, 1)).astype(jnp.bfloat16)
    g_out = dot(o_t, d_mid_full, (1, 0)).astype(jnp.bfloat16)
    d_qkv_t = attn_bwd(qkv_t, o_t, do_t, lse, cuts, dim)
    g_qkv_t = dot(d_qkv_t, attn_in, (1, 0)).astype(jnp.bfloat16)
    g_qkv = jnp.transpose(g_qkv_t.reshape(1, 3, dim, hidden), (3, 0, 1, 2))
    d_attn_part = dot(d_qkv_t, w_qkv_t, (0, 0)).astype(jnp.bfloat16)
    d_attn_in = lax.psum_scatter(d_attn_part, 'model', scatter_dimension=0, tiled=True)
    d_x_ln, d_gain_attn = ln1_vjp(d_attn_in.astype(jnp.float32))
    grad_in = (d_mid.astype(jnp.float32) + d_x_ln).astype(jnp.bfloat16)
    gain_sums = lax.psum(jnp.stack([d_gain_attn, d_gain_mlp]), 'model')
    return (hidden_out[None], grad_in[None], g_qkv, g_out[None], g_up, g_down, gain_sums[0].astype(jnp.bfloat16), gain_sums[1].astype(jnp.bfloat16))


def solution(mesh):
    act_spec = P('data', 'model', None)
    in_specs = (act_spec, P('data', None), P(), P(None, 'model', None, None), P('model', None, None), P(), P(None, 'model'), P('model', None), act_spec)
    out_specs = (act_spec, act_spec, P('data', 'model', None, None), P(('data', 'model'), None, None), P('data', 'model'), P(('data', 'model'), None), P('data'), P('data'))
    return jax.shard_map(local_layer, mesh=mesh, in_specs=in_specs, out_specs=out_specs, check_vma=False)
```
